1024 devices in a mesh: gx: 4 (over y_lo), gy: 16 (over z), gz: 16 (over x, y_hi, core).
Axes of the slice: x: 4, y: 8 (y_hi: 2, y_lo: 4; y = y_hi * 4 + y_lo), z: 16, core: 2. Of those that a mesh axis runs over, the one named last changes fastest.
Arguments:
- positions: float32 [4, 16, 16, 3, 48], P('gx', 'gy', 'gz'), may hold values from 0 to 1
- species: int32 [4, 16, 16, 48], P('gx', 'gy', 'gz'), may hold values from 0 to 3
- neighbours: int32 [4, 16, 16, 48, 128], P('gx', 'gy', 'gz'), may hold values from 0 to 1295
- neigh_counts: int32 [4, 16, 16, 48], P('gx', 'gy', 'gz'), may hold values from 64 to 128
- embedding: bfloat16 [4, 128], replicated, may hold values from -6 to 6
- rbf_decay: float32 [16], replicated, may hold values from 0.2 to 5
- radial_weight: bfloat16 [2, 16, 128], replicated, may hold values from -1.5 to 1.5
- node_weight: bfloat16 [2, 128, 128], replicated, may hold values from -0.5 to 0.5
- readout: bfloat16 [128], replicated, may hold values from -0.5 to 0.5
- species_bias: float32 [4], replicated, may hold values from -4 to 4
Outputs:
- atom_energy: float32 [4, 16, 16, 48], P('gx', 'gy', 'gz')
- total_energy: float32 [], replicated
The draws below stay inside these ranges and needn't reach their ends.
Inputs may be any that keep to these rules, and one draw needn't show every extreme that they name: `neighbours`: the offset code of an entry is 9 (dx + 1) + 3 (dy + 1) + (dz + 1) for a cell offset of -1, 0 or 1 along each dimension.
All inputs are finite; a program needn't handle non-finite values.
Results may differ from the reference program's by a relative error of at most 0.0028.
Values may be sent and summed in bfloat16 or wider, within the bound.
No kernel may reach another device: no remote copies, remote signals or barrier semaphores. Data moves between devices by JAX's collectives and lax.ppermute only.
A program may use at most 32 MiB of HBM per device.

```python
import math
import jax
import jax.numpy as jnp
from jax import lax

F = 128
NB = 128
NRBF = 16
NSPEC = 4
SLOTS = 48
LAYERS = 2
NX = 4
NY = 16
NZ = 16


def plant(result, key, least, largest):
    extent = result.shape
    spot = [jax.random.randint(jax.random.fold_in(key, axis), (), 0, extent[axis]) for axis in range(len(extent))]
    result = result.at[tuple(spot)].set(least)
    longest = extent.index(max(extent))
    spot[longest] = (spot[longest] + 1) % extent[longest]
    return result.at[tuple(spot)].set(largest)


def block_levels(rng, shape, cuts, smallest, top_value):
    loudness = 1.0
    for dim, blocks in cuts:
        draws = jax.random.uniform(jax.random.fold_in(jax.random.fold_in(rng, 6), dim), (blocks,), jnp.float32, smallest / len(cuts), top_value / len(cuts))
        loudness = loudness * jnp.repeat(jnp.exp(draws), shape[dim] // blocks).reshape((-1,) + (1,) * (len(shape) - 1 - dim))
    return loudness


def bell_draw(stream_key, shape, spread, most, kind=jnp.bfloat16):
    entries = spread * jax.random.normal(stream_key, shape, jnp.float32)
    return jnp.clip(entries, min=-most, max=most).astype(kind)


def setup_inputs(seed: int = 0) -> dict:
    splits = jax.random.split(jax.random.key(seed), 11)
    return {
        "positions": jnp.clip(1.0 * jax.random.uniform(splits[0], (NX, NY, NZ, 3, SLOTS), jnp.float32) ** block_levels(splits[0], (NX, NY, NZ, 3, SLOTS), ((0, 4), (1, 16), (2, 16)), -0.2, 0.2), 0.0, 1.0),
        "species": plant(jax.random.randint(splits[1], (NX, NY, NZ, SLOTS), 0, NSPEC), jax.random.fold_in(splits[1], 1), 0, NSPEC - 1).astype(jnp.int32),
        "neighbours": plant(jax.random.randint(splits[2], (NX, NY, NZ, SLOTS, NB), 0, 27 * SLOTS), jax.random.fold_in(splits[2], 1), 0, (27 * SLOTS) - 1).astype(jnp.int32),
        "neigh_counts": plant(jax.random.randint(splits[3], (NX, NY, NZ, SLOTS), NB // 2, NB + 1), jax.random.fold_in(splits[3], 1), NB // 2, NB).astype(jnp.int32),
        "embedding": bell_draw(splits[4], (NSPEC, F), 1.0, 6.0),
        "rbf_decay": jnp.clip(jnp.exp(jax.random.uniform(splits[5], (NRBF,), jnp.float32, math.log(0.2), math.log(5.0))), 0.2, 5.0),
        "radial_weight": bell_draw(splits[6], (LAYERS, NRBF, F), NRBF ** -0.5, 1.5),
        "node_weight": bell_draw(splits[7], (LAYERS, F, F), F ** -0.5, 0.5),
        "readout": bell_draw(splits[8], (F,), F ** -0.5, 0.5),
        "species_bias": bell_draw(splits[9], (NSPEC,), 1.0, 4.0, jnp.float32),
    }


def embed_atoms(species, embedding):
    kind_count = embedding.shape[0]
    one_hot = (species[..., None] == jnp.arange(kind_count, dtype=jnp.int32)).astype(jnp.bfloat16)
    embedded = jnp.dot(one_hot.reshape(-1, kind_count), embedding, preferred_element_type=jnp.float32)
    return embedded.astype(jnp.bfloat16).reshape(species.shape + (embedding.shape[1],))

def interaction(hidden_slab, place_slab, neighbour_row, count_row, rbf_decay, radial_weight, node_weight):
    cell_count, slot_count, neighbour_count = neighbour_row.shape
    feature_width = hidden_slab.shape[-1]
    slab_depth = cell_count + 2
    code_offset = neighbour_row // slot_count
    slot_index = neighbour_row % slot_count
    shift_x = code_offset // 9
    shift_y = code_offset // 3 % 3
    shift_z = code_offset % 3
    cell_column = lax.broadcasted_iota(jnp.int32, neighbour_row.shape, 0)
    cell_index = ((shift_x * 3 + shift_y) * slab_depth + cell_column + shift_z).reshape(-1)
    slot_flat = slot_index.reshape(-1)
    neighbour_feats = jnp.take(hidden_slab.reshape(-1, feature_width), cell_index * slot_count + slot_flat, axis=0)
    place_flat = place_slab.reshape(9 * slab_depth, 3, slot_count)
    far_place = place_flat[cell_index, :, slot_flat]
    centre = jnp.transpose(place_slab[1, 1, 1:slab_depth - 1], (0, 2, 1))
    offsets_xyz = jnp.stack([shift_x - 1, shift_y - 1, shift_z - 1], axis=-1).astype(jnp.float32)
    displace = far_place.reshape(cell_count, slot_count, neighbour_count, 3) + offsets_xyz - centre[:, :, None, :]
    distance_sq = lax.optimization_barrier(jnp.sum(displace * displace, axis=-1))
    radial_basis = jnp.exp(-distance_sq[..., None] * rbf_decay).astype(jnp.bfloat16).reshape(-1, rbf_decay.shape[0])
    filters = jnp.dot(radial_basis, radial_weight, preferred_element_type=jnp.float32)
    live_mask = (lax.broadcasted_iota(jnp.int32, neighbour_row.shape, 2) < count_row[:, :, None]).reshape(-1, 1)
    terms = jnp.where(live_mask, filters * neighbour_feats.astype(jnp.float32), jnp.float32(0.0))
    message = terms.reshape(cell_count * slot_count, neighbour_count, feature_width).sum(axis=1)
    inv_scale = lax.rsqrt(lax.optimization_barrier(jnp.mean(message * message, axis=-1, keepdims=True)) + 1e-05)
    normed = (message * inv_scale).astype(jnp.bfloat16)
    update = jax.nn.silu(jnp.dot(normed, node_weight, preferred_element_type=jnp.float32))
    own_rows = hidden_slab[1, 1, 1:slab_depth - 1].reshape(-1, feature_width).astype(jnp.float32)
    return (own_rows + update).astype(jnp.bfloat16).reshape(cell_count, slot_count, feature_width)

def run_layer(hidden_pad, place_pad, neighbours, neigh_counts, rbf_decay, radial_weight, node_weight):
    span_x = neighbours.shape[0]
    span_y = neighbours.shape[1]

    def one_row(row_index):
        row_x = row_index // span_y
        row_y = row_index % span_y
        hidden_slab = lax.dynamic_slice_in_dim(lax.dynamic_slice_in_dim(hidden_pad, row_x, 3, 0), row_y, 3, 1)
        place_slab = lax.dynamic_slice_in_dim(lax.dynamic_slice_in_dim(place_pad, row_x, 3, 0), row_y, 3, 1)
        return interaction(hidden_slab, place_slab, neighbours[row_x, row_y], neigh_counts[row_x, row_y], rbf_decay, radial_weight, node_weight)
    row_results = lax.map(one_row, jnp.arange(span_x * span_y, dtype=jnp.int32))
    return row_results.reshape((span_x, span_y) + row_results.shape[1:])

def atom_energies(hidden, species, readout, species_bias):
    per_atom = lax.optimization_barrier(jnp.sum(hidden.astype(jnp.float32) * readout.astype(jnp.float32), axis=-1))
    one_hot = (species[..., None] == jnp.arange(species_bias.shape[0], dtype=jnp.int32)).astype(jnp.float32)
    return per_atom + lax.optimization_barrier(jnp.sum(one_hot * species_bias, axis=-1))

def reference(positions, species, neighbours, neigh_counts, embedding, rbf_decay, radial_weight, node_weight, readout, species_bias):
    pad_spec = ((1, 1), (1, 1), (1, 1), (0, 0), (0, 0))
    place_pad = jnp.pad(positions, pad_spec, mode='wrap')
    hidden = embed_atoms(species, embedding)
    for layer_index in range(LAYERS):
        hidden_pad = jnp.pad(hidden, pad_spec, mode='wrap')
        hidden = run_layer(hidden_pad, place_pad, neighbours, neigh_counts, rbf_decay, radial_weight[layer_index], node_weight[layer_index])
    energy = atom_energies(hidden, species, readout, species_bias)
    return (energy, jnp.sum(energy))
```

```python
import jax
import jax.numpy as jnp
from jax import lax
from jax.experimental import pallas as pl
from jax.experimental.pallas import tpu as pltpu
from jax.sharding import PartitionSpec as P

F = 128
NB = 128
NRBF = 16
SLOTS = 48
LAYERS = 2
PLANE = 9 * SLOTS
LANES = 512
TILES = 3 * LANES // 128
AXES = ("gx", "gy", "gz")
SMALL = pltpu.CompilerParams(vmem_limit_bytes=16 * 1024 * 1024)


def kept(array):
    return pltpu.with_memory_space_constraint(array, pltpu.VMEM)


def count_kernel(neighbours, counts, out, high, low, table):
    code = neighbours[...]
    offset = (code * 1366) >> 16
    slot = code - offset * SLOTS
    across = (offset * 171) >> 9
    depth = (across * 171) >> 9
    column = (across - depth * 3) * 3 + depth
    place = (offset - across * 3) * LANES + column * SLOTS + slot
    high[...] = place >> 7
    low[...] = place & 127
    lane = lax.broadcasted_iota(jnp.int32, (1, NB), 1)
    tile_of = lax.broadcasted_iota(jnp.int32, (16, NB), 0)
    lane_of = lax.broadcasted_iota(jnp.int32, (128, NB), 0)
    for atom in range(SLOTS):
        tile = jnp.where(lane < counts[atom], high[atom : atom + 1], -1)
        left = jnp.where(tile == tile_of, 1.0, 0.0).astype(jnp.bfloat16)
        right = jnp.where(low[atom : atom + 1] == lane_of, 1.0, 0.0).astype(jnp.bfloat16)
        table[atom * 16 : atom * 16 + 16] = lax.dot_general(
            left, right, (((1,), (1,)), ((), ())), preferred_element_type=jnp.float32
        )
    for tile in range(TILES):
        out[:, tile * 128 : tile * 128 + 128] = table[pl.ds(tile, SLOTS, stride=16), :].astype(
            jnp.bfloat16
        )


def count_table(neighbours, counts):
    return pl.pallas_call(
        count_kernel,
        out_shape=pltpu.VMEM((SLOTS, 3 * LANES), jnp.bfloat16),
        in_specs=[
            pl.BlockSpec(memory_space=pltpu.VMEM),
            pl.BlockSpec(memory_space=pltpu.SMEM),
        ],
        out_specs=pl.BlockSpec(memory_space=pltpu.VMEM),
        scratch_shapes=[
            pltpu.VMEM((SLOTS, NB), jnp.int32),
            pltpu.VMEM((SLOTS, NB), jnp.int32),
            pltpu.VMEM((SLOTS * 16, 128), jnp.float32),
        ],
        compiler_params=SMALL,
        name="count_table",
    )(neighbours, counts)


def node_update(edges, tables, radial, weight):
    message = jnp.zeros((SLOTS, F), jnp.float32)
    gathered = None
    for z in range(3):
        part = jnp.dot(
            edges[:, z * LANES : z * LANES + PLANE],
            tables[z],
            preferred_element_type=jnp.float32,
        )
        gathered = part if gathered is None else gathered + part
    weights = radial[...].astype(jnp.float32)
    for b in range(NRBF):
        message = message + gathered[b * SLOTS : (b + 1) * SLOTS] * weights[b : b + 1]
    scale = lax.rsqrt(jnp.mean(message * message, axis=1, keepdims=True) + 1e-05)
    normed = (message * scale).astype(jnp.bfloat16)
    moved = jnp.dot(normed, weight[...], preferred_element_type=jnp.float32)
    own = tables[1][4 * SLOTS : 5 * SLOTS].astype(jnp.float32)
    return (own + moved / (1.0 + jnp.exp(-moved))).astype(jnp.bfloat16)


def first_kernel(
    below, middle, above, counts, decay, embedding, radial, weight, edges, hidden
):
    kinds = embedding[...]
    kind_of = lax.broadcasted_iota(jnp.int32, (8, LANES), 0).astype(jnp.float32)
    cell = lax.broadcasted_iota(jnp.int32, (4, LANES), 1) // SLOTS
    part_of = lax.broadcasted_iota(jnp.int32, (4, LANES), 0)
    centre = jnp.transpose(middle[4])
    tables = []
    for z, records in enumerate((below, middle, above)):
        pieces = [records[c] for c in range(9)]
        pieces.append(jnp.zeros((4, LANES - PLANE), jnp.float32))
        rows = jnp.concatenate(pieces, axis=1)
        shift = jnp.where(part_of == 0, cell % 3 - 1, jnp.where(part_of == 1, cell // 3 - 1, z - 1))
        moved = rows + shift.astype(jnp.float32)
        squared = None
        for d in range(3):
            away = moved[d : d + 1] - centre[:, d : d + 1]
            squared = away * away if squared is None else squared + away * away
        times = counts[:, z * LANES : (z + 1) * LANES]
        for b in range(NRBF):
            basis = jnp.exp(squared * (-decay[b])).astype(jnp.bfloat16)
            edges[b * SLOTS : (b + 1) * SLOTS, z * LANES : (z + 1) * LANES] = basis * times
        one_hot = jnp.where(rows[3:4] == kind_of, 1.0, 0.0)
        one_hot = jnp.transpose(one_hot).astype(jnp.bfloat16)
        table = jnp.dot(one_hot, kinds, preferred_element_type=jnp.float32)
        tables.append(table[:PLANE].astype(jnp.bfloat16))
    hidden[...] = node_update(edges, tables, radial, weight)


def first_layer(records, counts, decay, embedding, radial, weight):
    vmem = pl.BlockSpec(memory_space=pltpu.VMEM)
    smem = pl.BlockSpec(memory_space=pltpu.SMEM)
    return pl.pallas_call(
        first_kernel,
        out_shape=(
            pltpu.VMEM((NRBF * SLOTS, 3 * LANES), jnp.bfloat16),
            pltpu.VMEM((SLOTS, F), jnp.bfloat16),
        ),
        in_specs=[vmem, vmem, vmem, vmem, smem, vmem, vmem, vmem],
        out_specs=(vmem, vmem),
        compiler_params=SMALL,
        name="first_layer",
    )(*map(kept, records), kept(counts), decay, embedding, radial, weight)


def second_kernel(
    edges, below, middle, above, radial, weight, readout, species, bias, energy, total
):
    tables = [below[...], middle[...], above[...]]
    hidden = node_update(edges, tables, radial, weight)
    terms = hidden.astype(jnp.float32) * readout[...].astype(jnp.float32)
    per_atom = jnp.sum(jnp.transpose(terms), axis=0, keepdims=True)
    kind = species[...]
    offset = jnp.zeros((1, SLOTS), jnp.float32)
    for k in range(4):
        offset = offset + jnp.where(kind == k, bias[k], 0.0)
    result = per_atom + offset
    energy[...] = result
    total[...] = jnp.broadcast_to(jnp.sum(result, axis=1, keepdims=True), (1, 128))


def second_layer(edges, tables, radial, weight, readout, species, bias):
    vmem = pl.BlockSpec(memory_space=pltpu.VMEM)
    smem = pl.BlockSpec(memory_space=pltpu.SMEM)
    return pl.pallas_call(
        second_kernel,
        out_shape=(
            jax.ShapeDtypeStruct((1, SLOTS), jnp.float32),
            jax.ShapeDtypeStruct((1, 128), jnp.float32),
        ),
        in_specs=[vmem, vmem, vmem, vmem, vmem, vmem, vmem, vmem, smem],
        out_specs=(vmem, vmem),
        compiler_params=SMALL,
        name="second_layer",
    )(kept(edges), *map(kept, tables), radial, weight, readout, species, bias)


def both_ways(block, axis):
    count = lax.axis_size(axis)
    forward = [(i, (i + 1) % count) for i in range(count)]
    backward = [(target, source) for source, target in forward]
    return lax.ppermute(block, axis, forward), block, lax.ppermute(block, axis, backward)


def halo(block):
    row = jnp.concatenate(both_ways(block[None], "gx"), axis=0)
    sheet = jnp.concatenate(both_ways(row[None], "gy"), axis=0)
    return both_ways(sheet, "gz")


def summed(row):
    for axis in AXES:
        copies = jnp.broadcast_to(row[None], (lax.axis_size(axis),) + row.shape)
        row = jnp.sum(lax.all_to_all(copies, axis, 0, 0), axis=0)
    return row


def body(
    positions,
    species,
    neighbours,
    neigh_counts,
    embedding,
    rbf_decay,
    radial_weight,
    node_weight,
    readout,
    species_bias,
):
    kinds = species.reshape(1, SLOTS)
    records = jnp.concatenate([positions.reshape(3, SLOTS), kinds.astype(jnp.float32)], axis=0)
    counts = count_table(neighbours.reshape(SLOTS, NB), neigh_counts.reshape(SLOTS))
    places = [part.reshape(9, 4, SLOTS) for part in halo(records)]
    kinds_table = jnp.pad(embedding, ((0, 4), (0, 0)))
    edges, hidden = first_layer(
        places, counts, rbf_decay, kinds_table, radial_weight[0], node_weight[0]
    )
    tables = [part.reshape(PLANE, F) for part in halo(hidden)]
    energy, total = second_layer(
        edges, tables, radial_weight[1], node_weight[1], readout.reshape(1, F), kinds, species_bias
    )
    return energy.reshape(1, 1, 1, SLOTS), summed(total)[0, 0]


def solution(mesh):
    split = P("gx", "gy", "gz")
    in_specs = (split, split, split, split, P(), P(), P(), P(), P(), P())
    return jax.shard_map(
        body, mesh=mesh, in_specs=in_specs, out_specs=(split, P()), check_vma=False
    )
```

```python
import jax
import jax.numpy as jnp
from jax import lax
from jax.experimental import pallas as pl
from jax.experimental.pallas import tpu as pltpu
from jax.sharding import PartitionSpec as P

F = 128
NB = 128
NRBF = 16
SLOTS = 48
LAYERS = 2
PLANE = 9 * SLOTS
LANES = 512
TILES = 3 * LANES // 128
NX, NY, NZ = 4, 16, 16
SHEET = NX * NZ
AXES = ("gx", "gy", "gz")
SMALL = pltpu.CompilerParams(vmem_limit_bytes=16 * 1024 * 1024)
VMEM = pl.BlockSpec(memory_space=pltpu.VMEM)
HBM = pl.BlockSpec(memory_space=pltpu.HBM)


def side(axis):
    return 1 - 2 * (lax.axis_index(axis) & 1)


def kept(array):
    return pltpu.with_memory_space_constraint(array, pltpu.VMEM)


def outside(array):
    return pltpu.with_memory_space_constraint(array, pltpu.HBM)


def fetch(sources, targets, semaphores):
    copies = [
        pltpu.make_async_copy(source, target, semaphores.at[i])
        for i, (source, target) in enumerate(zip(sources, targets))
    ]
    for copy in copies:
        copy.start()
    for copy in copies:
        copy.wait()


def pack_kernel(positions, species, out, places, kinds, semaphores):
    fetch((positions, species), (places, kinds), semaphores)
    rows = [places[d] for d in range(3)] + [kinds[...].astype(jnp.float32)]
    record = jnp.concatenate(rows, axis=1)
    for i in range(SHEET):
        out[i] = record


def packed(positions, species):
    return pl.pallas_call(
        pack_kernel,
        out_shape=pltpu.VMEM((SHEET, 1, 4 * SLOTS), jnp.float32),
        in_specs=[HBM, HBM],
        out_specs=VMEM,
        scratch_shapes=[
            pltpu.VMEM((3, 1, SLOTS), jnp.float32),
            pltpu.VMEM((1, SLOTS), jnp.int32),
            pltpu.SemaphoreType.DMA((2,)),
        ],
        compiler_params=SMALL,
        name="pack_records",
    )(outside(positions), outside(species))


def pick_kernel(records, out):
    x = lax.axis_index("gx")
    z = lax.axis_index("gz")
    for i in range(3):
        row = (x + (i - 1) * side("gx")) & (NX - 1)
        for k in range(3):
            record = records[row * NZ + ((z + (k - 1) * side("gz")) & (NZ - 1))]
            for d in range(4):
                out[i * 3 + k, d : d + 1] = record[:, d * SLOTS : (d + 1) * SLOTS]


def picked(records):
    return pl.pallas_call(
        pick_kernel,
        out_shape=pltpu.VMEM((9, 4, SLOTS), jnp.float32),
        in_specs=[VMEM],
        out_specs=VMEM,
        compiler_params=SMALL,
        name="pick_records",
    )(kept(records))


def prepare_kernel(
    neighbours,
    neigh_counts,
    species,
    embedding,
    decay,
    radial,
    weight,
    readout,
    bias,
    out,
    rates,
    filters,
    updates,
    kinds,
    ends,
    codes,
    counts,
    kind,
    rows,
    scales,
    narrow,
    last,
    offsets,
    high,
    low,
    table,
    semaphores,
):
    fetch(
        (neighbours, neigh_counts, species, embedding, decay, radial, weight, readout, bias),
        (codes, counts, kind, rows, scales, narrow, updates, last, offsets),
        semaphores,
    )
    code = codes[...]
    offset = (code * 1366) >> 16
    slot = code - offset * SLOTS
    across = (offset * 171) >> 9
    depth = (across * 171) >> 9
    x = 1 + (depth - 1) * side("gx")
    y = 1 + (across - depth * 3 - 1) * side("gy")
    z = 1 + (offset - across * 3 - 1) * side("gz")
    place = y * LANES + (x * 3 + z) * SLOTS + slot
    high[...] = place >> 7
    low[...] = place & 127
    lane = lax.broadcasted_iota(jnp.int32, (1, NB), 1)
    tile_of = lax.broadcasted_iota(jnp.int32, (16, NB), 0)
    lane_of = lax.broadcasted_iota(jnp.int32, (128, NB), 0)
    for atom in range(SLOTS):
        tile = jnp.where(lane < counts[atom], high[atom : atom + 1], -1)
        left = jnp.where(tile == tile_of, 1.0, 0.0).astype(jnp.bfloat16)
        right = jnp.where(low[atom : atom + 1] == lane_of, 1.0, 0.0).astype(jnp.bfloat16)
        table[atom * 16 : atom * 16 + 16] = lax.dot_general(
            left, right, (((1,), (1,)), ((), ())), preferred_element_type=jnp.float32
        )
    for tile in range(TILES):
        out[:, tile * 128 : tile * 128 + 128] = table[pl.ds(tile, SLOTS, stride=16), :].astype(
            jnp.bfloat16
        )
    for b in range(NRBF):
        rates[b : b + 1] = jnp.full((1, LANES), -scales[b], jnp.float32)
    filters[...] = narrow[...].astype(jnp.float32)
    known = rows[...].astype(jnp.float32)
    kinds[...] = jnp.concatenate([known, jnp.zeros((4, F), jnp.float32)], axis=0).astype(
        jnp.bfloat16
    )
    ends[0:1] = last[...].astype(jnp.float32)
    shift = jnp.zeros((1, SLOTS), jnp.float32)
    for k in range(4):
        shift = shift + jnp.where(kind[...] == k, offsets[k], 0.0)
    ends[1:2, 0:SLOTS] = shift


def prepared(*arrays):
    return pl.pallas_call(
        prepare_kernel,
        out_shape=(
            pltpu.VMEM((SLOTS, 3 * LANES), jnp.bfloat16),
            pltpu.VMEM((NRBF, LANES), jnp.float32),
            pltpu.VMEM((LAYERS, NRBF, F), jnp.float32),
            pltpu.VMEM((LAYERS, F, F), jnp.bfloat16),
            pltpu.VMEM((8, F), jnp.bfloat16),
            pltpu.VMEM((2, F), jnp.float32),
        ),
        in_specs=[HBM] * 9,
        out_specs=(VMEM,) * 6,
        scratch_shapes=[
            pltpu.VMEM((SLOTS, NB), jnp.int32),
            pltpu.SMEM((SLOTS,), jnp.int32),
            pltpu.VMEM((1, SLOTS), jnp.int32),
            pltpu.VMEM((4, F), jnp.bfloat16),
            pltpu.SMEM((NRBF,), jnp.float32),
            pltpu.VMEM((LAYERS, NRBF, F), jnp.bfloat16),
            pltpu.VMEM((1, F), jnp.bfloat16),
            pltpu.SMEM((4,), jnp.float32),
            pltpu.VMEM((SLOTS, NB), jnp.int32),
            pltpu.VMEM((SLOTS, NB), jnp.int32),
            pltpu.VMEM((SLOTS * 16, 128), jnp.float32),
            pltpu.SemaphoreType.DMA((9,)),
        ],
        compiler_params=SMALL,
        name="prepare",
    )(*map(outside, arrays))


def node_update(edges, tables, weights, weight):
    message = jnp.zeros((SLOTS, F), jnp.float32)
    gathered = None
    for y in range(3):
        part = jnp.dot(
            edges[:, y * LANES : y * LANES + PLANE],
            tables[y],
            preferred_element_type=jnp.float32,
        )
        gathered = part if gathered is None else gathered + part
    for b in range(NRBF):
        message = message + gathered[b * SLOTS : (b + 1) * SLOTS] * weights[b : b + 1]
    scale = lax.rsqrt(jnp.mean(message * message, axis=1, keepdims=True) + 1e-05)
    normed = (message * scale).astype(jnp.bfloat16)
    moved = jnp.dot(normed, weight, preferred_element_type=jnp.float32)
    own = tables[1][4 * SLOTS : 5 * SLOTS].astype(jnp.float32)
    return (own + moved / (1.0 + jnp.exp(-moved))).astype(jnp.bfloat16)


def first_kernel(
    before, middle, after, counts, rates, embedding, radial, weight, edges, hidden
):
    kinds = embedding[...]
    kind_of = lax.broadcasted_iota(jnp.int32, (8, LANES), 0).astype(jnp.float32)
    cell = lax.broadcasted_iota(jnp.int32, (4, LANES), 1) // SLOTS
    part_of = lax.broadcasted_iota(jnp.int32, (4, LANES), 0)
    across = (cell // 3 - 1) * side("gx")
    along = (cell % 3 - 1) * side("gz")
    centre = jnp.transpose(middle[4])
    tables = []
    for y, records in enumerate((before, middle, after)):
        pieces = [records[c] for c in range(9)]
        pieces.append(jnp.zeros((4, LANES - PLANE), jnp.float32))
        rows = jnp.concatenate(pieces, axis=1)
        shift = jnp.where(
            part_of == 0, across, jnp.where(part_of == 1, (y - 1) * side("gy"), along)
        )
        moved = rows + shift.astype(jnp.float32)
        squared = None
        for d in range(3):
            away = moved[d : d + 1] - centre[:, d : d + 1]
            squared = away * away if squared is None else squared + away * away
        times = counts[:, y * LANES : (y + 1) * LANES]
        for b in range(NRBF):
            basis = jnp.exp(squared * rates[b : b + 1]).astype(jnp.bfloat16)
            edges[b * SLOTS : (b + 1) * SLOTS, y * LANES : (y + 1) * LANES] = basis * times
        one_hot = jnp.where(rows[3:4] == kind_of, 1.0, 0.0)
        one_hot = jnp.transpose(one_hot).astype(jnp.bfloat16)
        table = jnp.dot(one_hot, kinds, preferred_element_type=jnp.float32)
        tables.append(table[:PLANE].astype(jnp.bfloat16))
    hidden[0] = node_update(edges, tables, radial[0], weight[0])


def first_layer(records, counts, rates, embedding, radial, weight):
    return pl.pallas_call(
        first_kernel,
        out_shape=(
            pltpu.VMEM((NRBF * SLOTS, 3 * LANES), jnp.bfloat16),
            pltpu.VMEM((1, SLOTS, F), jnp.bfloat16),
        ),
        in_specs=[VMEM] * 8,
        out_specs=(VMEM, VMEM),
        compiler_params=SMALL,
        name="first_layer",
    )(*map(kept, (*records, counts, rates, embedding, radial, weight)))


def second_kernel(edges, before, middle, after, radial, weight, ends, energy, total):
    tables = [before[...], middle[...], after[...]]
    hidden = node_update(edges, tables, radial[1], weight[1])
    terms = hidden.astype(jnp.float32) * ends[0:1]
    per_atom = jnp.sum(jnp.transpose(terms), axis=0, keepdims=True)
    result = per_atom + ends[1:2, 0:SLOTS]
    energy[...] = result
    total[...] = jnp.broadcast_to(jnp.sum(result, axis=1, keepdims=True), (1, 128))


def second_layer(edges, tables, radial, weight, ends):
    return pl.pallas_call(
        second_kernel,
        out_shape=(
            jax.ShapeDtypeStruct((1, SLOTS), jnp.float32),
            pltpu.VMEM((1, 128), jnp.float32),
        ),
        in_specs=[VMEM] * 7,
        out_specs=(VMEM, VMEM),
        compiler_params=SMALL,
        name="second_layer",
    )(*map(kept, (edges, *tables, radial, weight, ends)))


def both_sides(block, axis):
    count = lax.axis_size(axis)
    near = [(i, i ^ 1) for i in range(count)]
    far = [(i, (i - 1 + 2 * (i & 1)) % count) for i in range(count)]
    return lax.ppermute(block, axis, far), block, lax.ppermute(block, axis, near)


def halo(block):
    line = jnp.concatenate(both_sides(block, "gz"), axis=0)
    sheet = jnp.concatenate(both_sides(line[None], "gx"), axis=0)
    return both_sides(sheet, "gy")


def summed(row):
    for axes in (("gx", "gz"), ("gy",)):
        copies = jnp.broadcast_to(row[None], (lax.axis_size(axes),) + row.shape)
        row = jnp.sum(lax.all_to_all(copies, axes, 0, 0), axis=0)
    return row


def body(
    positions,
    species,
    neighbours,
    neigh_counts,
    embedding,
    rbf_decay,
    radial_weight,
    node_weight,
    readout,
    species_bias,
):
    kinds = species.reshape(1, SLOTS)
    records = packed(positions.reshape(3, 1, SLOTS), kinds)
    records = picked(lax.all_to_all(records, ("gx", "gz"), 0, 0))
    places = both_sides(records, "gy")
    counts, rates, filters, updates, embedded, ends = prepared(
        neighbours.reshape(SLOTS, NB),
        neigh_counts.reshape(SLOTS),
        kinds,
        embedding,
        rbf_decay,
        radial_weight,
        node_weight,
        readout.reshape(1, F),
        species_bias,
    )
    edges, hidden = first_layer(places, counts, rates, embedded, filters, updates)
    tables = [part.reshape(PLANE, F) for part in halo(hidden)]
    energy, total = second_layer(edges, tables, filters, updates, ends)
    return energy.reshape(1, 1, 1, SLOTS), summed(total)[0, 0]


def solution(mesh):
    split = P("gx", "gy", "gz")
    in_specs = (split, split, split, split, P(), P(), P(), P(), P(), P())
    return jax.shard_map(
        body, mesh=mesh, in_specs=in_specs, out_specs=(split, P()), check_vma=False
    )
```

```python
import jax
import jax.numpy as jnp
from jax import lax
from jax.experimental import pallas as pl
from jax.experimental.pallas import tpu as pltpu
from jax.sharding import PartitionSpec as P

F = 128
NB = 128
NRBF = 16
SLOTS = 48
LAYERS = 2
PLANE = 9 * SLOTS
LANES = 512
TILES = 3 * LANES // 128
NX, NY, NZ = 4, 16, 16
SHEET = NX * NZ
AXES = ("gx", "gy", "gz")
SMALL = pltpu.CompilerParams(vmem_limit_bytes=16 * 1024 * 1024)
VMEM = pl.BlockSpec(memory_space=pltpu.VMEM)
HBM = pl.BlockSpec(memory_space=pltpu.HBM)


def side(axis):
    return 2 * (lax.axis_index(axis) & 1) - 1


def kept(array):
    return pltpu.with_memory_space_constraint(array, pltpu.VMEM)


def outside(array):
    return pltpu.with_memory_space_constraint(array, pltpu.HBM)


def fetch(sources, targets, semaphores):
    copies = [
        pltpu.make_async_copy(source, target, semaphores.at[i])
        for i, (source, target) in enumerate(zip(sources, targets))
    ]
    for copy in copies:
        copy.start()
    for copy in copies:
        copy.wait()


def pack_kernel(positions, species, out, places, kinds, semaphores):
    fetch((positions, species), (places, kinds), semaphores)
    rows = [places[d] for d in range(3)] + [kinds[...].astype(jnp.float32)]
    record = jnp.concatenate(rows, axis=1)
    for i in range(SHEET):
        out[i] = record


def packed(positions, species):
    return pl.pallas_call(
        pack_kernel,
        out_shape=pltpu.VMEM((SHEET, 1, 4 * SLOTS), jnp.float32),
        in_specs=[HBM, HBM],
        out_specs=VMEM,
        scratch_shapes=[
            pltpu.VMEM((3, 1, SLOTS), jnp.float32),
            pltpu.VMEM((1, SLOTS), jnp.int32),
            pltpu.SemaphoreType.DMA((2,)),
        ],
        compiler_params=SMALL,
        name="pack_records",
    )(outside(positions), outside(species))


def pick_kernel(records, out):
    x = lax.axis_index("gx")
    z = lax.axis_index("gz")
    for i in range(3):
        row = (x + (i - 1) * side("gx")) & (NX - 1)
        for k in range(3):
            record = records[row * NZ + ((z + (k - 1) * side("gz")) & (NZ - 1))]
            for d in range(4):
                out[i * 3 + k, d : d + 1] = record[:, d * SLOTS : (d + 1) * SLOTS]


def picked(records):
    return pl.pallas_call(
        pick_kernel,
        out_shape=pltpu.VMEM((9, 4, SLOTS), jnp.float32),
        in_specs=[VMEM],
        out_specs=VMEM,
        compiler_params=SMALL,
        name="pick_records",
    )(kept(records))


def prepare_kernel(
    neighbours,
    neigh_counts,
    species,
    embedding,
    decay,
    radial,
    weight,
    readout,
    bias,
    out,
    rates,
    filters,
    updates,
    kinds,
    ends,
    codes,
    counts,
    kind,
    rows,
    scales,
    narrow,
    last,
    offsets,
    high,
    low,
    table,
    semaphores,
):
    fetch(
        (neighbours, neigh_counts, species, embedding, decay, radial, weight, readout, bias),
        (codes, counts, kind, rows, scales, narrow, updates, last, offsets),
        semaphores,
    )
    code = codes[...]
    offset = (code * 1366) >> 16
    slot = code - offset * SLOTS
    across = (offset * 171) >> 9
    depth = (across * 171) >> 9
    x = 1 + (depth - 1) * side("gx")
    y = 1 + (across - depth * 3 - 1) * side("gy")
    z = 1 + (offset - across * 3 - 1) * side("gz")
    place = y * LANES + (x * 3 + z) * SLOTS + slot
    high[...] = place >> 7
    low[...] = place & 127
    lane = lax.broadcasted_iota(jnp.int32, (1, NB), 1)
    tile_of = lax.broadcasted_iota(jnp.int32, (16, NB), 0)
    lane_of = lax.broadcasted_iota(jnp.int32, (128, NB), 0)
    for atom in range(SLOTS):
        tile = jnp.where(lane < counts[atom], high[atom : atom + 1], -1)
        left = jnp.where(tile == tile_of, 1.0, 0.0).astype(jnp.bfloat16)
        right = jnp.where(low[atom : atom + 1] == lane_of, 1.0, 0.0).astype(jnp.bfloat16)
        table[atom * 16 : atom * 16 + 16] = lax.dot_general(
            left, right, (((1,), (1,)), ((), ())), preferred_element_type=jnp.float32
        )
    for tile in range(TILES):
        out[:, tile * 128 : tile * 128 + 128] = table[pl.ds(tile, SLOTS, stride=16), :].astype(
            jnp.bfloat16
        )
    for b in range(NRBF):
        rates[b : b + 1] = jnp.full((1, LANES), -scales[b], jnp.float32)
    filters[...] = narrow[...].astype(jnp.float32)
    known = rows[...].astype(jnp.float32)
    kinds[...] = jnp.concatenate([known, jnp.zeros((4, F), jnp.float32)], axis=0).astype(
        jnp.bfloat16
    )
    ends[0:1] = last[...].astype(jnp.float32)
    shift = jnp.zeros((1, SLOTS), jnp.float32)
    for k in range(4):
        shift = shift + jnp.where(kind[...] == k, offsets[k], 0.0)
    ends[1:2, 0:SLOTS] = shift


def prepared(*arrays):
    return pl.pallas_call(
        prepare_kernel,
        out_shape=(
            pltpu.VMEM((SLOTS, 3 * LANES), jnp.bfloat16),
            pltpu.VMEM((NRBF, LANES), jnp.float32),
            pltpu.VMEM((LAYERS, NRBF, F), jnp.float32),
            pltpu.VMEM((LAYERS, F, F), jnp.bfloat16),
            pltpu.VMEM((8, F), jnp.bfloat16),
            pltpu.VMEM((2, F), jnp.float32),
        ),
        in_specs=[HBM] * 9,
        out_specs=(VMEM,) * 6,
        scratch_shapes=[
            pltpu.VMEM((SLOTS, NB), jnp.int32),
            pltpu.SMEM((SLOTS,), jnp.int32),
            pltpu.VMEM((1, SLOTS), jnp.int32),
            pltpu.VMEM((4, F), jnp.bfloat16),
            pltpu.SMEM((NRBF,), jnp.float32),
            pltpu.VMEM((LAYERS, NRBF, F), jnp.bfloat16),
            pltpu.VMEM((1, F), jnp.bfloat16),
            pltpu.SMEM((4,), jnp.float32),
            pltpu.VMEM((SLOTS, NB), jnp.int32),
            pltpu.VMEM((SLOTS, NB), jnp.int32),
            pltpu.VMEM((SLOTS * 16, 128), jnp.float32),
            pltpu.SemaphoreType.DMA((9,)),
        ],
        compiler_params=SMALL,
        name="prepare",
    )(*map(outside, arrays))


def node_update(edges, tables, weights, weight):
    message = jnp.zeros((SLOTS, F), jnp.float32)
    gathered = None
    for y in range(3):
        part = jnp.dot(
            edges[:, y * LANES : y * LANES + PLANE],
            tables[y],
            preferred_element_type=jnp.float32,
        )
        gathered = part if gathered is None else gathered + part
    for b in range(NRBF):
        message = message + gathered[b * SLOTS : (b + 1) * SLOTS] * weights[b : b + 1]
    scale = lax.rsqrt(jnp.mean(message * message, axis=1, keepdims=True) + 1e-05)
    normed = (message * scale).astype(jnp.bfloat16)
    moved = jnp.dot(normed, weight, preferred_element_type=jnp.float32)
    own = tables[1][4 * SLOTS : 5 * SLOTS].astype(jnp.float32)
    return (own + moved / (1.0 + jnp.exp(-moved))).astype(jnp.bfloat16)


def first_kernel(
    before, middle, after, counts, rates, embedding, radial, weight, edges, hidden
):
    kinds = embedding[...]
    kind_of = lax.broadcasted_iota(jnp.int32, (8, LANES), 0).astype(jnp.float32)
    cell = lax.broadcasted_iota(jnp.int32, (4, LANES), 1) // SLOTS
    part_of = lax.broadcasted_iota(jnp.int32, (4, LANES), 0)
    across = (cell // 3 - 1) * side("gx")
    along = (cell % 3 - 1) * side("gz")
    centre = jnp.transpose(middle[4])
    tables = []
    for y, records in enumerate((before, middle, after)):
        pieces = [records[c] for c in range(9)]
        pieces.append(jnp.zeros((4, LANES - PLANE), jnp.float32))
        rows = jnp.concatenate(pieces, axis=1)
        shift = jnp.where(
            part_of == 0, across, jnp.where(part_of == 1, (y - 1) * side("gy"), along)
        )
        moved = rows + shift.astype(jnp.float32)
        squared = None
        for d in range(3):
            away = moved[d : d + 1] - centre[:, d : d + 1]
            squared = away * away if squared is None else squared + away * away
        times = counts[:, y * LANES : (y + 1) * LANES]
        for b in range(NRBF):
            basis = jnp.exp(squared * rates[b : b + 1]).astype(jnp.bfloat16)
            edges[b * SLOTS : (b + 1) * SLOTS, y * LANES : (y + 1) * LANES] = basis * times
        one_hot = jnp.where(rows[3:4] == kind_of, 1.0, 0.0)
        one_hot = jnp.transpose(one_hot).astype(jnp.bfloat16)
        table = jnp.dot(one_hot, kinds, preferred_element_type=jnp.float32)
        tables.append(table[:PLANE].astype(jnp.bfloat16))
    hidden[0] = node_update(edges, tables, radial[0], weight[0])


def first_layer(records, counts, rates, embedding, radial, weight):
    return pl.pallas_call(
        first_kernel,
        out_shape=(
            pltpu.VMEM((NRBF * SLOTS, 3 * LANES), jnp.bfloat16),
            pltpu.VMEM((1, SLOTS, F), jnp.bfloat16),
        ),
        in_specs=[VMEM] * 8,
        out_specs=(VMEM, VMEM),
        compiler_params=SMALL,
        name="first_layer",
    )(*map(kept, (*records, counts, rates, embedding, radial, weight)))


def second_kernel(edges, before, middle, after, radial, weight, ends, energy, total):
    tables = [before[...], middle[...], after[...]]
    hidden = node_update(edges, tables, radial[1], weight[1])
    terms = hidden.astype(jnp.float32) * ends[0:1]
    per_atom = jnp.sum(jnp.transpose(terms), axis=0, keepdims=True)
    result = per_atom + ends[1:2, 0:SLOTS]
    energy[...] = result
    total[...] = jnp.broadcast_to(jnp.sum(result, axis=1, keepdims=True), (1, 128))


def second_layer(edges, tables, radial, weight, ends):
    return pl.pallas_call(
        second_kernel,
        out_shape=(
            jax.ShapeDtypeStruct((1, SLOTS), jnp.float32),
            pltpu.VMEM((1, 128), jnp.float32),
        ),
        in_specs=[VMEM] * 7,
        out_specs=(VMEM, VMEM),
        compiler_params=SMALL,
        name="second_layer",
    )(*map(kept, (edges, *tables, radial, weight, ends)))


def both_sides(block, axis):
    count = lax.axis_size(axis)
    near = [(i, i ^ 1) for i in range(count)]
    far = [(i, (i - 1 + 2 * (i & 1)) % count) for i in range(count)]
    return lax.ppermute(block, axis, near), block, lax.ppermute(block, axis, far)


def halo(block):
    line = jnp.concatenate(both_sides(block, "gz"), axis=0)
    sheet = jnp.concatenate(both_sides(line[None], "gx"), axis=0)
    return both_sides(sheet, "gy")


def summed(row):
    for axes in (("gx", "gz"), ("gy",)):
        copies = jnp.broadcast_to(row[None], (lax.axis_size(axes),) + row.shape)
        row = jnp.sum(lax.all_to_all(copies, axes, 0, 0), axis=0)
    return row


def body(
    positions,
    species,
    neighbours,
    neigh_counts,
    embedding,
    rbf_decay,
    radial_weight,
    node_weight,
    readout,
    species_bias,
):
    kinds = species.reshape(1, SLOTS)
    records = packed(positions.reshape(3, 1, SLOTS), kinds)
    records = picked(lax.all_to_all(records, ("gx", "gz"), 0, 0))
    places = both_sides(records, "gy")
    counts, rates, filters, updates, embedded, ends = prepared(
        neighbours.reshape(SLOTS, NB),
        neigh_counts.reshape(SLOTS),
        kinds,
        embedding,
        rbf_decay,
        radial_weight,
        node_weight,
        readout.reshape(1, F),
        species_bias,
    )
    edges, hidden = first_layer(places, counts, rates, embedded, filters, updates)
    tables = [part.reshape(PLANE, F) for part in halo(hidden)]
    energy, total = second_layer(edges, tables, filters, updates, ends)
    return energy.reshape(1, 1, 1, SLOTS), summed(total)[0, 0]


def solution(mesh):
    split = P("gx", "gy", "gz")
    in_specs = (split, split, split, split, P(), P(), P(), P(), P(), P())
    return jax.shard_map(
        body, mesh=mesh, in_specs=in_specs, out_specs=(split, P()), check_vma=False
    )
```

```python
import jax
import jax.numpy as jnp
from jax import lax
from jax.experimental import pallas as pl
from jax.experimental.pallas import tpu as pltpu
from jax.sharding import PartitionSpec as P

F = 128
NB = 128
NRBF = 16
SLOTS = 48
LAYERS = 2
PLANE = 9 * SLOTS
LANES = 512
TILES = 3 * LANES // 128
NX, NY, NZ = 4, 16, 16
SHEET = NX * NZ
AXES = ("gx", "gy", "gz")
SMALL = pltpu.CompilerParams(vmem_limit_bytes=16 * 1024 * 1024)
VMEM = pl.BlockSpec(memory_space=pltpu.VMEM)
HBM = pl.BlockSpec(memory_space=pltpu.HBM)


def side(axis):
    return 2 * (lax.axis_index(axis) & 1) - 1


def kept(array):
    return pltpu.with_memory_space_constraint(array, pltpu.VMEM)


def outside(array):
    return pltpu.with_memory_space_constraint(array, pltpu.HBM)


def fetch(sources, targets, semaphores):
    copies = [
        pltpu.make_async_copy(source, target, semaphores.at[i])
        for i, (source, target) in enumerate(zip(sources, targets))
    ]
    for copy in copies:
        copy.start()
    for copy in copies:
        copy.wait()


def pack_kernel(positions, species, out, places, kinds, semaphores):
    fetch((positions, species), (places, kinds), semaphores)
    rows = [places[d] for d in range(3)] + [kinds[...].astype(jnp.float32)]
    record = jnp.concatenate(rows, axis=1)
    for i in range(SHEET):
        out[i] = record


def packed(positions, species):
    return pl.pallas_call(
        pack_kernel,
        out_shape=pltpu.VMEM((SHEET, 1, 4 * SLOTS), jnp.float32),
        in_specs=[HBM, HBM],
        out_specs=VMEM,
        scratch_shapes=[
            pltpu.VMEM((3, 1, SLOTS), jnp.float32),
            pltpu.VMEM((1, SLOTS), jnp.int32),
            pltpu.SemaphoreType.DMA((2,)),
        ],
        compiler_params=SMALL,
        name="pack_records",
    )(outside(positions), outside(species))


def pick_kernel(records, out):
    x = lax.axis_index("gx")
    z = lax.axis_index("gz")
    for i in range(3):
        row = (x + (i - 1) * side("gx")) & (NX - 1)
        for k in range(3):
            record = records[row * NZ + ((z + (k - 1) * side("gz")) & (NZ - 1))]
            for d in range(4):
                out[i * 3 + k, d : d + 1] = record[:, d * SLOTS : (d + 1) * SLOTS]


def picked(records):
    return pl.pallas_call(
        pick_kernel,
        out_shape=pltpu.VMEM((9, 4, SLOTS), jnp.float32),
        in_specs=[VMEM],
        out_specs=VMEM,
        compiler_params=SMALL,
        name="pick_records",
    )(kept(records))


def prepare_kernel(
    neighbours,
    neigh_counts,
    species,
    embedding,
    decay,
    radial,
    weight,
    readout,
    bias,
    out,
    rates,
    filters,
    updates,
    kinds,
    ends,
    codes,
    counts,
    kind,
    rows,
    scales,
    narrow,
    last,
    offsets,
    high,
    low,
    table,
    semaphores,
):
    fetch(
        (neighbours, neigh_counts, species, embedding, decay, radial, weight, readout, bias),
        (codes, counts, kind, rows, scales, narrow, updates, last, offsets),
        semaphores,
    )
    code = codes[...]
    offset = (code * 1366) >> 16
    slot = code - offset * SLOTS
    across = (offset * 171) >> 9
    depth = (across * 171) >> 9
    x = 1 + (depth - 1) * side("gx")
    y = 1 + (across - depth * 3 - 1) * side("gy")
    z = 1 + (offset - across * 3 - 1) * side("gz")
    place = y * LANES + (x * 3 + z) * SLOTS + slot
    high[...] = place >> 7
    low[...] = place & 127
    lane = lax.broadcasted_iota(jnp.int32, (1, NB), 1)
    tile_of = lax.broadcasted_iota(jnp.int32, (16, NB), 0)
    lane_of = lax.broadcasted_iota(jnp.int32, (128, NB), 0)
    for atom in range(SLOTS):
        tile = jnp.where(lane < counts[atom], high[atom : atom + 1], -1)
        left = jnp.where(tile == tile_of, 1.0, 0.0).astype(jnp.bfloat16)
        right = jnp.where(low[atom : atom + 1] == lane_of, 1.0, 0.0).astype(jnp.bfloat16)
        table[atom * 16 : atom * 16 + 16] = lax.dot_general(
            left, right, (((1,), (1,)), ((), ())), preferred_element_type=jnp.float32
        )
    for tile in range(TILES):
        out[:, tile * 128 : tile * 128 + 128] = table[pl.ds(tile, SLOTS, stride=16), :].astype(
            jnp.bfloat16
        )
    for b in range(NRBF):
        rates[b : b + 1] = jnp.full((1, LANES), -scales[b], jnp.float32)
    filters[...] = narrow[...].astype(jnp.float32)
    known = rows[...].astype(jnp.float32)
    kinds[...] = jnp.concatenate([known, jnp.zeros((4, F), jnp.float32)], axis=0).astype(
        jnp.bfloat16
    )
    ends[0:1] = last[...].astype(jnp.float32)
    shift = jnp.zeros((1, SLOTS), jnp.float32)
    for k in range(4):
        shift = shift + jnp.where(kind[...] == k, offsets[k], 0.0)
    ends[1:2, 0:SLOTS] = shift


def prepared(*arrays):
    return pl.pallas_call(
        prepare_kernel,
        out_shape=(
            pltpu.VMEM((SLOTS, 3 * LANES), jnp.bfloat16),
            pltpu.VMEM((NRBF, LANES), jnp.float32),
            pltpu.VMEM((LAYERS, NRBF, F), jnp.float32),
            pltpu.VMEM((LAYERS, F, F), jnp.bfloat16),
            pltpu.VMEM((8, F), jnp.bfloat16),
            pltpu.VMEM((2, F), jnp.float32),
        ),
        in_specs=[HBM] * 9,
        out_specs=(VMEM,) * 6,
        scratch_shapes=[
            pltpu.VMEM((SLOTS, NB), jnp.int32),
            pltpu.SMEM((SLOTS,), jnp.int32),
            pltpu.VMEM((1, SLOTS), jnp.int32),
            pltpu.VMEM((4, F), jnp.bfloat16),
            pltpu.SMEM((NRBF,), jnp.float32),
            pltpu.VMEM((LAYERS, NRBF, F), jnp.bfloat16),
            pltpu.VMEM((1, F), jnp.bfloat16),
            pltpu.SMEM((4,), jnp.float32),
            pltpu.VMEM((SLOTS, NB), jnp.int32),
            pltpu.VMEM((SLOTS, NB), jnp.int32),
            pltpu.VMEM((SLOTS * 16, 128), jnp.float32),
            pltpu.SemaphoreType.DMA((9,)),
        ],
        compiler_params=SMALL,
        name="prepare",
    )(*map(outside, arrays))


def node_update(edges, tables, weights, weight):
    message = jnp.zeros((SLOTS, F), jnp.float32)
    gathered = None
    for y in range(3):
        part = jnp.dot(
            edges[:, y * LANES : y * LANES + PLANE],
            tables[y],
            preferred_element_type=jnp.float32,
        )
        gathered = part if gathered is None else gathered + part
    for b in range(NRBF):
        message = message + gathered[b * SLOTS : (b + 1) * SLOTS] * weights[b : b + 1]
    scale = lax.rsqrt(jnp.mean(message * message, axis=1, keepdims=True) + 1e-05)
    normed = (message * scale).astype(jnp.bfloat16)
    moved = jnp.dot(normed, weight, preferred_element_type=jnp.float32)
    own = tables[1][4 * SLOTS : 5 * SLOTS].astype(jnp.float32)
    return (own + moved / (1.0 + jnp.exp(-moved))).astype(jnp.bfloat16)


def first_kernel(
    before, middle, after, counts, rates, embedding, radial, weight, edges, hidden
):
    kinds = embedding[...]
    kind_of = lax.broadcasted_iota(jnp.int32, (8, LANES), 0).astype(jnp.float32)
    cell = lax.broadcasted_iota(jnp.int32, (4, LANES), 1) // SLOTS
    part_of = lax.broadcasted_iota(jnp.int32, (4, LANES), 0)
    across = (cell // 3 - 1) * side("gx")
    along = (cell % 3 - 1) * side("gz")
    centre = jnp.transpose(middle[4])
    tables = []
    for y, records in enumerate((before, middle, after)):
        pieces = [records[c] for c in range(9)]
        pieces.append(jnp.zeros((4, LANES - PLANE), jnp.float32))
        rows = jnp.concatenate(pieces, axis=1)
        shift = jnp.where(
            part_of == 0, across, jnp.where(part_of == 1, (y - 1) * side("gy"), along)
        )
        moved = rows + shift.astype(jnp.float32)
        squared = None
        for d in range(3):
            away = moved[d : d + 1] - centre[:, d : d + 1]
            squared = away * away if squared is None else squared + away * away
        times = counts[:, y * LANES : (y + 1) * LANES]
        for b in range(NRBF):
            basis = jnp.exp(squared * rates[b : b + 1]).astype(jnp.bfloat16)
            edges[b * SLOTS : (b + 1) * SLOTS, y * LANES : (y + 1) * LANES] = basis * times
        one_hot = jnp.where(rows[3:4] == kind_of, 1.0, 0.0)
        one_hot = jnp.transpose(one_hot).astype(jnp.bfloat16)
        table = jnp.dot(one_hot, kinds, preferred_element_type=jnp.float32)
        tables.append(table[:PLANE].astype(jnp.bfloat16))
    hidden[0] = node_update(edges, tables, radial[0], weight[0])


def first_layer(records, counts, rates, embedding, radial, weight):
    return pl.pallas_call(
        first_kernel,
        out_shape=(
            pltpu.VMEM((NRBF * SLOTS, 3 * LANES), jnp.bfloat16),
            pltpu.VMEM((1, SLOTS, F), jnp.bfloat16),
        ),
        in_specs=[VMEM] * 8,
        out_specs=(VMEM, VMEM),
        compiler_params=SMALL,
        name="first_layer",
    )(*map(kept, (*records, counts, rates, embedding, radial, weight)))


def second_kernel(edges, before, middle, after, radial, weight, ends, energy, total):
    tables = [before[...], middle[...], after[...]]
    hidden = node_update(edges, tables, radial[1], weight[1])
    terms = hidden.astype(jnp.float32) * ends[0:1]
    per_atom = jnp.sum(jnp.transpose(terms), axis=0, keepdims=True)
    result = per_atom + ends[1:2, 0:SLOTS]
    energy[...] = result
    total[...] = jnp.broadcast_to(jnp.sum(result, axis=1, keepdims=True), (1, 128))


def second_layer(edges, tables, radial, weight, ends):
    return pl.pallas_call(
        second_kernel,
        out_shape=(
            jax.ShapeDtypeStruct((1, SLOTS), jnp.float32),
            pltpu.VMEM((1, 128), jnp.float32),
        ),
        in_specs=[VMEM] * 7,
        out_specs=(VMEM, VMEM),
        compiler_params=SMALL,
        name="second_layer",
    )(*map(kept, (edges, *tables, radial, weight, ends)))


def both_sides(block, axis):
    count = lax.axis_size(axis)
    near = [(i, i ^ 1) for i in range(count)]
    far = [(i, (i - 1 + 2 * (i & 1)) % count) for i in range(count)]
    return lax.ppermute(block, axis, near), block, lax.ppermute(block, axis, far)


def halo(block):
    line = jnp.concatenate(both_sides(block, "gz"), axis=0)
    sheet = jnp.concatenate(both_sides(line[None], "gx"), axis=0)
    return both_sides(sheet, "gy")


def summed(row):
    for axes in (("gy",), ("gx", "gz")):
        copies = jnp.broadcast_to(row[None], (lax.axis_size(axes),) + row.shape)
        row = jnp.sum(lax.all_to_all(copies, axes, 0, 0), axis=0)
    return row


def body(
    positions,
    species,
    neighbours,
    neigh_counts,
    embedding,
    rbf_decay,
    radial_weight,
    node_weight,
    readout,
    species_bias,
):
    kinds = species.reshape(1, SLOTS)
    records = packed(positions.reshape(3, 1, SLOTS), kinds)
    records = picked(lax.all_to_all(records, ("gx", "gz"), 0, 0))
    places = both_sides(records, "gy")
    counts, rates, filters, updates, embedded, ends = prepared(
        neighbours.reshape(SLOTS, NB),
        neigh_counts.reshape(SLOTS),
        kinds,
        embedding,
        rbf_decay,
        radial_weight,
        node_weight,
        readout.reshape(1, F),
        species_bias,
    )
    edges, hidden = first_layer(places, counts, rates, embedded, filters, updates)
    tables = [part.reshape(PLANE, F) for part in halo(hidden)]
    energy, total = second_layer(edges, tables, filters, updates, ends)
    return energy.reshape(1, 1, 1, SLOTS), summed(total)[0, 0]


def solution(mesh):
    split = P("gx", "gy", "gz")
    in_specs = (split, split, split, split, P(), P(), P(), P(), P(), P())
    return jax.shard_map(
        body, mesh=mesh, in_specs=in_specs, out_specs=(split, P()), check_vma=False
    )
```

```python
import jax
import jax.numpy as jnp
from jax import lax
from jax.experimental import pallas as pl
from jax.experimental.pallas import tpu as pltpu
from jax.sharding import PartitionSpec as P

F = 128
NB = 128
NRBF = 16
SLOTS = 48
LAYERS = 2
PLANE = 9 * SLOTS
LANES = 512
TILES = 3 * LANES // 128
NX, NY, NZ = 4, 16, 16
SHEET = NX * NZ
AXES = ("gx", "gy", "gz")
SMALL = pltpu.CompilerParams(vmem_limit_bytes=16 * 1024 * 1024)
VMEM = pl.BlockSpec(memory_space=pltpu.VMEM)
HBM = pl.BlockSpec(memory_space=pltpu.HBM)


def side(axis):
    return 2 * (lax.axis_index(axis) & 1) - 1


def kept(array):
    return pltpu.with_memory_space_constraint(array, pltpu.VMEM)


def outside(array):
    return pltpu.with_memory_space_constraint(array, pltpu.HBM)


def fetch(sources, targets, semaphores):
    copies = [
        pltpu.make_async_copy(source, target, semaphores.at[i])
        for i, (source, target) in enumerate(zip(sources, targets))
    ]
    for copy in copies:
        copy.start()
    for copy in copies:
        copy.wait()


def pack_kernel(positions, species, out, places, kinds, semaphores):
    fetch((positions, species), (places, kinds), semaphores)
    rows = [places[d] for d in range(3)] + [kinds[...].astype(jnp.float32)]
    record = jnp.concatenate(rows, axis=1)
    for i in range(SHEET):
        out[i] = record


def packed(positions, species):
    return pl.pallas_call(
        pack_kernel,
        out_shape=pltpu.VMEM((SHEET, 1, 4 * SLOTS), jnp.float32),
        in_specs=[HBM, HBM],
        out_specs=VMEM,
        scratch_shapes=[
            pltpu.VMEM((3, 1, SLOTS), jnp.float32),
            pltpu.VMEM((1, SLOTS), jnp.int32),
            pltpu.SemaphoreType.DMA((2,)),
        ],
        compiler_params=SMALL,
        name="pack_records",
    )(outside(positions), outside(species))


def pick_kernel(records, out):
    x = lax.axis_index("gx")
    z = lax.axis_index("gz")
    for i in range(3):
        row = (x + (i - 1) * side("gx")) & (NX - 1)
        for k in range(3):
            record = records[row * NZ + ((z + (k - 1) * side("gz")) & (NZ - 1))]
            for d in range(4):
                out[k * 3 + i, d : d + 1] = record[:, d * SLOTS : (d + 1) * SLOTS]


def picked(records):
    return pl.pallas_call(
        pick_kernel,
        out_shape=pltpu.VMEM((9, 4, SLOTS), jnp.float32),
        in_specs=[VMEM],
        out_specs=VMEM,
        compiler_params=SMALL,
        name="pick_records",
    )(kept(records))


def prepare_kernel(
    neighbours,
    neigh_counts,
    species,
    embedding,
    decay,
    radial,
    weight,
    readout,
    bias,
    out,
    rates,
    filters,
    updates,
    kinds,
    ends,
    codes,
    counts,
    kind,
    rows,
    scales,
    narrow,
    last,
    offsets,
    high,
    low,
    table,
    semaphores,
):
    fetch(
        (neighbours, neigh_counts, species, embedding, decay, radial, weight, readout, bias),
        (codes, counts, kind, rows, scales, narrow, updates, last, offsets),
        semaphores,
    )
    code = codes[...]
    offset = (code * 1366) >> 16
    slot = code - offset * SLOTS
    across = (offset * 171) >> 9
    depth = (across * 171) >> 9
    x = 1 + (depth - 1) * side("gx")
    y = 1 + (across - depth * 3 - 1) * side("gy")
    z = 1 + (offset - across * 3 - 1) * side("gz")
    place = y * LANES + (z * 3 + x) * SLOTS + slot
    high[...] = place >> 7
    low[...] = place & 127
    lane = lax.broadcasted_iota(jnp.int32, (1, NB), 1)
    tile_of = lax.broadcasted_iota(jnp.int32, (16, NB), 0)
    lane_of = lax.broadcasted_iota(jnp.int32, (128, NB), 0)
    for atom in range(SLOTS):
        tile = jnp.where(lane < counts[atom], high[atom : atom + 1], -1)
        left = jnp.where(tile == tile_of, 1.0, 0.0).astype(jnp.bfloat16)
        right = jnp.where(low[atom : atom + 1] == lane_of, 1.0, 0.0).astype(jnp.bfloat16)
        table[atom * 16 : atom * 16 + 16] = lax.dot_general(
            left, right, (((1,), (1,)), ((), ())), preferred_element_type=jnp.float32
        )
    for tile in range(TILES):
        out[:, tile * 128 : tile * 128 + 128] = table[pl.ds(tile, SLOTS, stride=16), :].astype(
            jnp.bfloat16
        )
    for b in range(NRBF):
        rates[b : b + 1] = jnp.full((1, LANES), -scales[b], jnp.float32)
    filters[...] = narrow[...].astype(jnp.float32)
    known = rows[...].astype(jnp.float32)
    kinds[...] = jnp.concatenate([known, jnp.zeros((4, F), jnp.float32)], axis=0).astype(
        jnp.bfloat16
    )
    ends[0:1] = last[...].astype(jnp.float32)
    shift = jnp.zeros((1, SLOTS), jnp.float32)
    for k in range(4):
        shift = shift + jnp.where(kind[...] == k, offsets[k], 0.0)
    ends[1:2, 0:SLOTS] = shift


def prepared(*arrays):
    return pl.pallas_call(
        prepare_kernel,
        out_shape=(
            pltpu.VMEM((SLOTS, 3 * LANES), jnp.bfloat16),
            pltpu.VMEM((NRBF, LANES), jnp.float32),
            pltpu.VMEM((LAYERS, NRBF, F), jnp.float32),
            pltpu.VMEM((LAYERS, F, F), jnp.bfloat16),
            pltpu.VMEM((8, F), jnp.bfloat16),
            pltpu.VMEM((2, F), jnp.float32),
        ),
        in_specs=[HBM] * 9,
        out_specs=(VMEM,) * 6,
        scratch_shapes=[
            pltpu.VMEM((SLOTS, NB), jnp.int32),
            pltpu.SMEM((SLOTS,), jnp.int32),
            pltpu.VMEM((1, SLOTS), jnp.int32),
            pltpu.VMEM((4, F), jnp.bfloat16),
            pltpu.SMEM((NRBF,), jnp.float32),
            pltpu.VMEM((LAYERS, NRBF, F), jnp.bfloat16),
            pltpu.VMEM((1, F), jnp.bfloat16),
            pltpu.SMEM((4,), jnp.float32),
            pltpu.VMEM((SLOTS, NB), jnp.int32),
            pltpu.VMEM((SLOTS, NB), jnp.int32),
            pltpu.VMEM((SLOTS * 16, 128), jnp.float32),
            pltpu.SemaphoreType.DMA((9,)),
        ],
        compiler_params=SMALL,
        name="prepare",
    )(*map(outside, arrays))


def node_update(edges, tables, weights, weight):
    message = jnp.zeros((SLOTS, F), jnp.float32)
    gathered = None
    for y in range(3):
        part = jnp.dot(
            edges[:, y * LANES : y * LANES + PLANE],
            tables[y],
            preferred_element_type=jnp.float32,
        )
        gathered = part if gathered is None else gathered + part
    for b in range(NRBF):
        message = message + gathered[b * SLOTS : (b + 1) * SLOTS] * weights[b : b + 1]
    scale = lax.rsqrt(jnp.mean(message * message, axis=1, keepdims=True) + 1e-05)
    normed = (message * scale).astype(jnp.bfloat16)
    moved = jnp.dot(normed, weight, preferred_element_type=jnp.float32)
    own = tables[1][4 * SLOTS : 5 * SLOTS].astype(jnp.float32)
    return (own + moved / (1.0 + jnp.exp(-moved))).astype(jnp.bfloat16)


def first_kernel(
    before, middle, after, counts, rates, embedding, radial, weight, edges, hidden
):
    kinds = embedding[...]
    kind_of = lax.broadcasted_iota(jnp.int32, (8, LANES), 0).astype(jnp.float32)
    cell = lax.broadcasted_iota(jnp.int32, (4, LANES), 1) // SLOTS
    part_of = lax.broadcasted_iota(jnp.int32, (4, LANES), 0)
    across = (cell % 3 - 1) * side("gx")
    along = (cell // 3 - 1) * side("gz")
    centre = jnp.transpose(middle[4])
    tables = []
    for y, records in enumerate((before, middle, after)):
        pieces = [records[c] for c in range(9)]
        pieces.append(jnp.zeros((4, LANES - PLANE), jnp.float32))
        rows = jnp.concatenate(pieces, axis=1)
        shift = jnp.where(
            part_of == 0, across, jnp.where(part_of == 1, (y - 1) * side("gy"), along)
        )
        moved = rows + shift.astype(jnp.float32)
        squared = None
        for d in range(3):
            away = moved[d : d + 1] - centre[:, d : d + 1]
            squared = away * away if squared is None else squared + away * away
        times = counts[:, y * LANES : (y + 1) * LANES]
        for b in range(NRBF):
            basis = jnp.exp(squared * rates[b : b + 1]).astype(jnp.bfloat16)
            edges[b * SLOTS : (b + 1) * SLOTS, y * LANES : (y + 1) * LANES] = basis * times
        one_hot = jnp.where(rows[3:4] == kind_of, 1.0, 0.0)
        one_hot = jnp.transpose(one_hot).astype(jnp.bfloat16)
        table = jnp.dot(one_hot, kinds, preferred_element_type=jnp.float32)
        tables.append(table[:PLANE].astype(jnp.bfloat16))
    hidden[0] = node_update(edges, tables, radial[0], weight[0])


def first_layer(records, counts, rates, embedding, radial, weight):
    return pl.pallas_call(
        first_kernel,
        out_shape=(
            pltpu.VMEM((NRBF * SLOTS, 3 * LANES), jnp.bfloat16),
            pltpu.VMEM((1, SLOTS, F), jnp.bfloat16),
        ),
        in_specs=[VMEM] * 8,
        out_specs=(VMEM, VMEM),
        compiler_params=SMALL,
        name="first_layer",
    )(*map(kept, (*records, counts, rates, embedding, radial, weight)))


def second_kernel(edges, before, middle, after, radial, weight, ends, energy, total):
    tables = [before[...], middle[...], after[...]]
    hidden = node_update(edges, tables, radial[1], weight[1])
    terms = hidden.astype(jnp.float32) * ends[0:1]
    per_atom = jnp.sum(jnp.transpose(terms), axis=0, keepdims=True)
    result = per_atom + ends[1:2, 0:SLOTS]
    energy[...] = result
    total[...] = jnp.broadcast_to(jnp.sum(result, axis=1, keepdims=True), (1, 128))


def second_layer(edges, tables, radial, weight, ends):
    return pl.pallas_call(
        second_kernel,
        out_shape=(
            jax.ShapeDtypeStruct((1, SLOTS), jnp.float32),
            pltpu.VMEM((1, 128), jnp.float32),
        ),
        in_specs=[VMEM] * 7,
        out_specs=(VMEM, VMEM),
        compiler_params=SMALL,
        name="second_layer",
    )(*map(kept, (edges, *tables, radial, weight, ends)))


def both_sides(block, axis):
    count = lax.axis_size(axis)
    near = [(i, i ^ 1) for i in range(count)]
    far = [(i, (i - 1 + 2 * (i & 1)) % count) for i in range(count)]
    return lax.ppermute(block, axis, near), block, lax.ppermute(block, axis, far)


def halo(block):
    line = jnp.concatenate(both_sides(block, "gx"), axis=0)
    sheet = jnp.concatenate(both_sides(line[None], "gz"), axis=0)
    return both_sides(sheet, "gy")


def summed(row):
    for axes in (("gx", "gz"), ("gy",)):
        copies = jnp.broadcast_to(row[None], (lax.axis_size(axes),) + row.shape)
        row = jnp.sum(lax.all_to_all(copies, axes, 0, 0), axis=0)
    return row


def body(
    positions,
    species,
    neighbours,
    neigh_counts,
    embedding,
    rbf_decay,
    radial_weight,
    node_weight,
    readout,
    species_bias,
):
    kinds = species.reshape(1, SLOTS)
    records = packed(positions.reshape(3, 1, SLOTS), kinds)
    records = picked(lax.all_to_all(records, ("gx", "gz"), 0, 0))
    places = both_sides(records, "gy")
    counts, rates, filters, updates, embedded, ends = prepared(
        neighbours.reshape(SLOTS, NB),
        neigh_counts.reshape(SLOTS),
        kinds,
        embedding,
        rbf_decay,
        radial_weight,
        node_weight,
        readout.reshape(1, F),
        species_bias,
    )
    edges, hidden = first_layer(places, counts, rates, embedded, filters, updates)
    tables = [part.reshape(PLANE, F) for part in halo(hidden)]
    energy, total = second_layer(edges, tables, filters, updates, ends)
    return energy.reshape(1, 1, 1, SLOTS), summed(total)[0, 0]


def solution(mesh):
    split = P("gx", "gy", "gz")
    in_specs = (split, split, split, split, P(), P(), P(), P(), P(), P())
    return jax.shard_map(
        body, mesh=mesh, in_specs=in_specs, out_specs=(split, P()), check_vma=False
    )
```
